32 devices in a mesh: node: 4 (over y, x), row: 8 (over z, core).
Axes of the slice: x: 2, y: 2, z: 4, core: 2. Of those that a mesh axis runs over, the one named last changes fastest.
Arguments:
- inputs: float32 [16, 32, 128, 128], P(None, 'row'), may hold values from -8 to 8
- diagonal: float32 [32, 128, 128], P('row'), may hold values from 0.05 to 1
- observations: float32 [16, 32, 128, 128], P(None, 'row'), may hold values from -0.0078125 to 0.0078125
- frequencies: float32 [4], replicated, may hold values from 0.2 to 3
- weights: float32 [4], replicated, may hold values from 0.5 to 2
- counts: int32 [4], replicated, may hold values from 3 to 6, as said below
- assignment: int32 [4], replicated, may hold values from 0 to 3, each once
Outputs:
- probe_response: float32 [16, 32, 128, 128], P(None, 'row')
- group_gram: float32 [4, 16, 16], P('node')
The draws below stay inside these ranges and needn't reach their ends.
Inputs may be any that keep to these rules, and one draw needn't show every extreme that they name: `counts`: some node has 6 sweeps and some node 3 in every draw. `assignment`: each node 0 to 3 appears once.
All inputs are finite; a program needn't handle non-finite values.
Results may differ from the reference program's by a relative error of at most 0.0003.
Values sent between devices are 32-bit elements; how exact they have to be, the bound alone decides.
A program may use at most 192 MiB of HBM per device.

```python
import math
import jax
import jax.numpy as jnp
from jax import lax

INPUTS = 16
PROBES = 16
GY = 128
GZ = 128
NODE_DEV = 1
ITERS = 6
QUAD = 4
NX = 32
CELLS = 524288
N_NODE = 4


def draw_inputs(key, part):
    values = jnp.clip(2.0 * jax.random.normal(key, (INPUTS, NX, GY, GZ), jnp.float32), -8.0, 8.0)
    return values.astype(jnp.float32)


def draw_counts(key, part):
    first, second, third = jax.random.split(jax.random.fold_in(key, 17), 3)
    values = jax.random.randint(first, (QUAD,), ITERS // 2, ITERS + 1, jnp.int32)
    top_slot = jax.random.randint(second, (), 0, QUAD, jnp.int32)
    low_slot = (top_slot + 1 + jax.random.randint(third, (), 0, QUAD - 1, jnp.int32)) % QUAD
    values = values.at[top_slot].set(ITERS)
    values = values.at[low_slot].set(ITERS // 2)
    return values.astype(jnp.int32)


def block_scale(stream_key, extent, cuts, least, high):
    gain, own = 1.0, jax.random.fold_in(stream_key, 6)
    for position, blocks in cuts:
        heights = jnp.exp(jax.random.uniform(jax.random.fold_in(own, position), (blocks,), jnp.float32, least / len(cuts), high / len(cuts)))
        gain = gain * jnp.repeat(heights, extent[position] // blocks).reshape([-1 if axis == position else 1 for axis in range(len(extent))])
    return gain


def normal_values(own_key, shape, width, bound, pieces=(), kind=jnp.bfloat16):
    entries = jax.random.normal(own_key, shape, jnp.float32) * width
    if len(pieces) > 0:
        entries = block_scale(own_key, shape, pieces, -0.22, 0.18) * entries
    return jnp.clip(entries, min=-bound, max=bound).astype(kind)


def setup_inputs(seed: int = 0) -> dict:
    seeds = jax.random.split(jax.random.key(seed), 8)
    inputs = draw_inputs(jax.random.fold_in(seeds[7], 71), 0)
    diagonal = jnp.clip(jnp.exp(math.log(1.0) - 2.9957323 * jax.random.uniform(seeds[1], (NX, GY, GZ), jnp.float32) ** block_scale(seeds[1], (NX, GY, GZ), ((0, 8),), -0.2, 0.2)), 0.05, 1.0)
    observations = normal_values(seeds[2], (PROBES, NX, GY, GZ), CELLS ** -0.5, 0.0078125, ((1, 8),), jnp.float32)
    frequencies = jnp.clip(jax.random.uniform(seeds[3], (QUAD,), jnp.float32, 0.2, 3.0), 0.2, 3.0)
    weights = jnp.clip(jnp.exp(jax.random.uniform(seeds[4], (QUAD,), jnp.float32, math.log(0.5), math.log(2.0))), 0.5, 2.0)
    counts = draw_counts(jax.random.fold_in(seeds[7], 71), 0)
    assignment = jax.random.permutation(seeds[6], QUAD).astype(jnp.int32)
    return {"inputs": inputs, "diagonal": diagonal, "observations": observations, "frequencies": frequencies, "weights": weights, "counts": counts, "assignment": assignment}


def relax_step(fields, source, diagonal, shift_val, active):
    padded = jnp.pad(fields, ((0, 0), (0, 0), (1, 1), (1, 1), (1, 1)))
    beside = padded[:, :, 2:, 1:-1, 1:-1] + padded[:, :, :-2, 1:-1, 1:-1]
    beside = beside + padded[:, :, 1:-1, 2:, 1:-1] + padded[:, :, 1:-1, :-2, 1:-1]
    beside = beside + padded[:, :, 1:-1, 1:-1, 2:] + padded[:, :, 1:-1, 1:-1, :-2]
    diag_full = 6.0 + diagonal
    applied = diag_full * fields - beside
    resid_real = source - applied[0] + shift_val * fields[1]
    resid_imag = -applied[1] - shift_val * fields[0]
    denominator = diag_full * diag_full + shift_val * shift_val
    step_real = (diag_full * resid_real + shift_val * resid_imag) / denominator
    step_imag = (diag_full * resid_imag - shift_val * resid_real) / denominator
    return fields + active * jnp.stack([step_real, step_imag], 0)


def reference(inputs, diagonal, observations, frequencies, weights, counts, assignment):
    cells = NX * GY * GZ
    flat_probe = observations.reshape(PROBES, cells)

    def one_node(carry, node_id):
        shift_val = frequencies[node_id]
        fields = jnp.zeros((2,) + inputs.shape, jnp.float32)
        for sweep in range(ITERS):
            active = (sweep < counts[node_id]).astype(jnp.float32)
            fields = relax_step(fields, inputs, diagonal, shift_val, active)
        flat_fields = fields.reshape(2, INPUTS, cells)
        projected = jnp.einsum("aic,pc->aip", flat_fields, flat_probe, precision=lax.Precision.HIGHEST)
        gram_part = jnp.einsum("aic,ajc->ij", flat_fields, flat_fields, precision=lax.Precision.HIGHEST)
        contrib = jnp.einsum("aip,aic->pc", projected, flat_fields, precision=lax.Precision.HIGHEST)
        return carry + weights[node_id] * contrib, weights[node_id] * gram_part

    start = jnp.zeros((PROBES, cells), jnp.float32)
    total, grams = lax.scan(one_node, start, jnp.arange(QUAD, dtype=jnp.int32))
    probe_response = (total / QUAD).reshape(PROBES, NX, GY, GZ)
    group_gram = grams[assignment].reshape(N_NODE, NODE_DEV, INPUTS, INPUTS).sum(1) / cells
    return probe_response, group_gram
```

```python
import functools

import jax
import jax.numpy as jnp
from jax import lax
from jax.experimental import pallas as pl
from jax.experimental.pallas import tpu as pltpu
from jax.sharding import PartitionSpec as P

NODE_DEV = 1
ITERS = 6
VMEM_LIMIT = 62 * 1024 * 1024
STEP = 4


def sweep_kernel(halo, own, planes, counts_ref, freq_ref, obs_ref, *refs):
    pieces = refs[:-9]
    fhl_ref, acc_ref, src_ref, x_ref, f_ref, gr_ref, gi_ref, sems, obs_sem = refs[-9:]
    total = planes + 2 * halo
    win = own + 2 * halo
    cols, gz = src_ref.shape[2:]
    quad = counts_ref.shape[0]
    copies = []
    at = 0
    for n, piece in enumerate(pieces):
        copies.append(
            pltpu.make_async_copy(piece, src_ref.at[pl.ds(at, piece.shape[0])], sems.at[n])
        )
        at += piece.shape[0]
    for copy in copies:
        copy.start()
    for copy in copies:
        copy.wait()

    lane = lax.broadcasted_iota(jnp.int32, (cols, gz), 1)
    first = lane == 0
    last = lane == gz - 1

    def beside(v):
        return jnp.where(first, 0.0, pltpu.roll(v, 1, 1)) + jnp.where(
            last, 0.0, pltpu.roll(v, gz - 1, 1)
        )

    def gain(p, y):
        return (
            jnp.broadcast_to(gr_ref[p, pl.ds(y, 1), :], (cols, gz)),
            jnp.broadcast_to(gi_ref[p, pl.ds(y, 1), :], (cols, gz)),
        )

    def sweep(slot, radius, put):
        low = halo - radius
        groups = (own + 2 * radius + STEP - 1) // STEP

        def plane(p, c):
            def rows(j, c):
                y = low + STEP * j
                us = [x_ref[slot, 0, p, y - 1 + t] for t in range(STEP + 2)]
                ws = [x_ref[slot, 1, p, y - 1 + t] for t in range(STEP + 2)]
                for t in range(STEP):
                    nu = x_ref[slot, 0, p - 1, y + t] + x_ref[slot, 0, p + 1, y + t]
                    nw = x_ref[slot, 1, p - 1, y + t] + x_ref[slot, 1, p + 1, y + t]
                    nu = (nu + (us[t] + us[t + 2])) + (beside(us[t + 1]) + src_ref[p, y + t])
                    nw = (nw + (ws[t] + ws[t + 2])) + beside(ws[t + 1])
                    gr, gi = gain(p, y + t)
                    put(p, y + t, gr * nu - gi * nw, gr * nw + gi * nu)
                return c

            return lax.fori_loop(0, groups, rows, c)

        lax.fori_loop(low, low + planes + 2 * radius, plane, 0)

    def node(k, c):
        w = freq_ref[k]
        count = counts_ref[k]

        def gains(p, c):
            part = src_ref[p, win:, :, :].reshape(gr_ref.shape[1:])
            d = 6.0 + part
            inv = jnp.where(part > 0.0, 1.0 / (d * d + w * w), 0.0)
            gr_ref[p] = d * inv
            gi_ref[p] = -w * inv
            return c

        lax.fori_loop(0, total, gains, 0)

        low1 = halo + 1 - count
        groups1 = (own + 2 * (count - 1) + STEP - 1) // STEP

        def start_plane(p, c):
            def rows(j, c):
                y = low1 + STEP * j
                for t in range(STEP):
                    b = src_ref[p, y + t]
                    gr, gi = gain(p, y + t)
                    x_ref[1, 0, p, y + t] = gr * b
                    x_ref[1, 1, p, y + t] = gi * b
                return c

            return lax.fori_loop(0, groups1, rows, c)

        lax.fori_loop(low1, low1 + planes + 2 * (count - 1), start_plane, 0)

        def middle(s, c):
            slot = (s - 1) % 2

            def put(p, y, u, v):
                x_ref[1 - slot, 0, p, y] = u
                x_ref[1 - slot, 1, p, y] = v

            sweep(slot, count - s, put)
            return c

        lax.fori_loop(2, count, middle, 0)

        def put_last(p, y, u, v):
            row = (p - halo) * own + (y - halo)
            f_ref[row, k, 0] = u
            f_ref[row, k, 1] = v

        sweep((count - 1) % 2, 0, put_last)
        return c

    lax.fori_loop(0, quad, node, 0)

    nf = quad * 2 * cols
    acc_ref[...] = jnp.zeros_like(acc_ref)

    def products(j, c):
        his, los, ohis, olos = [], [], [], []
        for t in range(2):
            f = f_ref[2 * j + t].reshape(nf, gz)
            hi = f.astype(jnp.bfloat16)
            lo = (f - hi.astype(jnp.float32)).astype(jnp.bfloat16)
            o = obs_ref[2 * j + t]
            ohi = o.astype(jnp.bfloat16)
            olo = (o - ohi.astype(jnp.float32)).astype(jnp.bfloat16)
            fhl_ref[2 * j + t, :nf] = hi
            fhl_ref[2 * j + t, nf:] = lo
            his.append(hi)
            los.append(lo)
            ohis.append(ohi)
            olos.append(olo)
        hi = jnp.concatenate(his, 1)
        left = jnp.concatenate([hi, jnp.concatenate(ohis, 1), jnp.concatenate(olos, 1)], 0)
        right = jnp.concatenate([hi, jnp.concatenate(los, 1)], 0)
        acc_ref[...] += lax.dot_general(
            left, right, (((1,), (1,)), ((), ())), preferred_element_type=jnp.float32
        )
        return c

    lax.fori_loop(0, f_ref.shape[0] // 2, products, 0)


def response_kernel(pw_ref, fhl_ref, out_ref):
    probes = out_ref.shape[1]
    gz = out_ref.shape[2]
    hi, lo = split(pw_ref[...])
    pw = jnp.concatenate(
        [jnp.concatenate([hi, hi], 1), jnp.concatenate([lo, jnp.zeros_like(lo)], 1)], 0
    )

    def pair(j, c):
        right = jnp.concatenate([fhl_ref[2 * j], fhl_ref[2 * j + 1]], 1)
        both = jnp.dot(pw, right, preferred_element_type=jnp.float32)
        both = both[:probes] + both[probes:]
        out_ref[2 * j] = both[:, :gz]
        out_ref[2 * j + 1] = both[:, gz:]
        return c

    lax.fori_loop(0, out_ref.shape[0] // 2, pair, 0)


def split(v):
    hi = v.astype(jnp.bfloat16)
    return hi, (v - hi.astype(jnp.float32)).astype(jnp.bfloat16)


def local(inputs, diagonal, observations, frequencies, weights, counts, assignment):
    parts = lax.axis_size("node")
    part = lax.axis_index("node")
    cols, planes, gy, gz = inputs.shape
    probes = observations.shape[0]
    quad = frequencies.shape[0]
    own = gy // parts
    halo = ITERS - 1
    win = own + 2 * halo
    extra = -(-(win + STEP) // cols)
    nf = quad * 2 * cols
    local_rows = planes * own

    window = jnp.pad(inputs, ((0, 0), (0, 0), (halo, halo), (0, 0)))
    window = lax.dynamic_slice_in_dim(window, part * own, win, 2).transpose(1, 2, 0, 3)
    diag = jnp.pad(diagonal, ((0, 0), (halo, halo), (0, 0)))
    diag = lax.dynamic_slice_in_dim(diag, part * own, win, 1)
    diag = jnp.pad(diag, ((0, 0), (0, extra * cols - win), (0, 0)))
    packed = jnp.concatenate([window, diag.reshape(planes, extra, cols, gz)], 1)

    count = lax.axis_size("row")
    lows, highs = [], []
    for hop in range(1, -(-halo // planes) + 1):
        size = min(planes, halo - (hop - 1) * planes)
        up = [(i, i + hop) for i in range(count - hop)]
        down = [(j, i) for i, j in up]
        lows.insert(0, lax.ppermute(packed[planes - size :], "row", up))
        highs.append(lax.ppermute(packed[:size], "row", down))
    pieces = lows + [packed] + highs

    obs = lax.dynamic_slice_in_dim(observations, part * own, own, 2)
    obs = obs.transpose(1, 2, 0, 3).reshape(local_rows, probes, gz)

    total = planes + 2 * halo
    vmem = pl.BlockSpec(memory_space=pltpu.VMEM)
    smem = pl.BlockSpec(memory_space=pltpu.SMEM)
    fhl, acc = pl.pallas_call(
        functools.partial(sweep_kernel, halo, own, planes),
        out_shape=(
            jax.ShapeDtypeStruct((local_rows, 2 * nf, gz), jnp.bfloat16),
            jax.ShapeDtypeStruct((nf + 2 * probes, 2 * nf), jnp.float32),
        ),
        in_specs=[smem, smem, vmem] + [pl.BlockSpec(memory_space=pl.ANY)] * len(pieces),
        out_specs=(vmem, vmem),
        scratch_shapes=[
            pltpu.VMEM((total, win + extra, cols, gz), jnp.float32),
            pltpu.VMEM((2, 2, total, win + STEP, cols, gz), jnp.float32),
            pltpu.VMEM((local_rows, quad, 2, cols, gz), jnp.float32),
            pltpu.VMEM((total, extra * cols, gz), jnp.float32),
            pltpu.VMEM((total, extra * cols, gz), jnp.float32),
            pltpu.SemaphoreType.DMA((len(pieces),)),
            pltpu.SemaphoreType.DMA,
        ],
        compiler_params=pltpu.CompilerParams(vmem_limit_bytes=VMEM_LIMIT),
        name="sweeps",
    )(counts, frequencies, obs, *pieces)

    proj = acc[nf : nf + probes, :nf] + acc[nf + probes :, :nf] + acc[nf : nf + probes, nf:]
    proj = lax.psum(proj, ("node", "row"))
    scale = jnp.repeat(weights / quad, 2 * cols)
    pw = proj * scale[None, :]
    share = pl.pallas_call(
        response_kernel,
        out_shape=jax.ShapeDtypeStruct((local_rows, probes, gz), jnp.float32),
        in_specs=[vmem, vmem],
        out_specs=vmem,
        compiler_params=pltpu.CompilerParams(vmem_limit_bytes=VMEM_LIMIT),
        name="response",
    )(pw, fhl)
    full = lax.all_gather(share.reshape(planes, own, probes, gz), "node")
    probe_response = full.transpose(3, 1, 0, 2, 4).reshape(observations.shape)

    cross = acc[:nf, nf:]
    gram = (acc[:nf, :nf] + cross + cross.T).reshape(quad, 2, cols, quad, 2, cols)
    gram = jnp.stack([gram[k, 0, :, k, 0] + gram[k, 1, :, k, 1] for k in range(quad)])
    gram = lax.psum(gram, ("node", "row"))
    cells = planes * gy * gz * count
    mine = lax.dynamic_slice_in_dim(assignment, part * NODE_DEV, NODE_DEV)
    group_gram = jnp.sum(weights[mine][:, None, None] * gram[mine], 0) / cells
    return probe_response, group_gram[None]


def solution(mesh):
    placed = (
        P(None, "row", None, None),
        P("row", None, None),
        P(None, "row", None, None),
        P(),
        P(),
        P(),
        P(),
    )
    return jax.shard_map(
        local,
        mesh=mesh,
        in_specs=placed,
        out_specs=(P(None, "row", None, None), P("node", None, None)),
        check_vma=False,
    )
```
